16 devices in a mesh: dp: 1, tp: 16 (over x, y, z, core).
Axes of the slice: x: 2, y: 2, z: 2, core: 2. Of those that a mesh axis runs over, the one named last changes fastest.
Arguments:
- x: bfloat16 [2048, 8192], P('dp')
- w_gate: bfloat16 [8192, 49152], P(None, 'tp')
- w_up: bfloat16 [8192, 49152], P(None, 'tp')
- w_down: bfloat16 [49152, 8192], P('tp')
Outputs:
- output: bfloat16 [2048, 8192], P('dp')
All inputs are finite; a program needn't handle non-finite values.
Results may differ from the reference program's by a relative error of at most 0.016.
Values are sent between devices in bfloat16 or wider.
A program may use at most 2 GiB of HBM per device.

```python
import jax
import jax.numpy as jnp

ROWS = 2048
D = 8192
FF = 49152


def setup_inputs(seed: int = 0, part: int = 0) -> dict:
    kx, kg, ku, kd = jax.random.split(jax.random.key(seed), 4)
    drawn = {
        "x": jax.random.normal(jax.random.fold_in(kx, part), (ROWS, D), jnp.float32),
        "w_gate": jax.random.normal(kg, (D, FF), jnp.float32) * D**-0.5,
        "w_up": jax.random.normal(ku, (D, FF), jnp.float32) * D**-0.5,
        "w_down": jax.random.normal(kd, (FF, D), jnp.float32) * FF**-0.5,
    }
    return {k: v.astype(jnp.bfloat16) for k, v in drawn.items()}


def reference(x, w_gate, w_up, w_down):
    gate = jnp.dot(x, w_gate, preferred_element_type=jnp.float32)
    up = jnp.dot(x, w_up, preferred_element_type=jnp.float32)
    hidden = (jax.nn.silu(gate) * up).astype(jnp.bfloat16)
    return jnp.dot(hidden, w_down, preferred_element_type=jnp.float32).astype(jnp.bfloat16)
```

```python
import jax
import jax.numpy as jnp
from jax import lax
from jax.experimental import pallas as pl
from jax.experimental.pallas import tpu as pltpu
from jax.sharding import PartitionSpec as P

MESH = pl.DeviceIdType.MESH
BF16, F32 = jnp.bfloat16, jnp.float32

R = 512
H = R // 2
TN = 256
TD = 1024
PIECES = 4
ORDERS = ((8, 4, 2), (4, 2, 8), (2, 8, 4))
TILES = ((6, 5, 5), (5, 6, 5), (5, 5, 6), (6, 5, 5))


def part_columns():
    out, at = [], 0
    for tiles in TILES:
        piece = []
        for t in tiles:
            piece.append((at, t * 128))
            at += t * 128
        out.append(piece)
    return out


COLS = part_columns()


def kernel(
    x, wg, wu, wd, y,
    xb, gb, ub, db, h, acc, oth, r0, out, r1, r2, r3,
    xsem, gsem, usem, dsem, s0s, s0r, ss, rs, lsem,
):
    rows, d = x.shape
    nc = rows // R
    ng = wg.shape[1] // TN
    nd = d // TD
    me = lax.axis_index("tp")
    bit = {m: lax.rem(me // m, 2) for m in (1, 2, 4, 8)}
    peer = {m: me + m - 2 * m * bit[m] for m in (1, 2, 4, 8)}
    core = bit[1]

    def remote(src, dst, ssem, rsem, mask):
        return pltpu.make_async_remote_copy(
            src_ref=src, dst_ref=dst, send_sem=ssem, recv_sem=rsem,
            device_id={"tp": peer[mask]}, device_id_type=MESH,
        )

    def load_x(c):
        own = pl.multiple_of(c * R + core * H, H)
        other = pl.multiple_of(c * R + (1 - core) * H, H)
        return (
            pltpu.make_async_copy(x.at[pl.ds(own, H)], xb.at[pl.ds(0, H)], xsem.at[0]),
            pltpu.make_async_copy(x.at[pl.ds(other, H)], xb.at[pl.ds(H, H)], xsem.at[1]),
        )

    def load_gu(j, slot):
        at = pl.ds(pl.multiple_of(j * TN, TN), TN)
        return (
            pltpu.make_async_copy(wg.at[:, at], gb.at[slot], gsem.at[slot]),
            pltpu.make_async_copy(wu.at[:, at], ub.at[slot], usem.at[slot]),
        )

    def load_d(k, slot):
        at = pl.ds(pl.multiple_of(k * TD, TD), TD)
        return (pltpu.make_async_copy(wd.at[:, at], db.at[slot], dsem.at[slot]),)

    def start(copies):
        for c in copies:
            c.start()

    def wait(copies):
        for c in copies:
            c.wait()

    def stage0(k):
        slot = lax.rem(k, 2)
        return remote(oth, r0.at[slot], s0s.at[slot], s0r.at[slot], 1)

    def finish0(k):
        stage0(k).wait()
        at = pl.ds(pl.multiple_of(k * TD, TD), TD)
        acc[:, at] = acc[:, at] + r0[lax.rem(k, 2)].astype(F32)

    def rows_at(c, order, depth):
        at, size = 0, H
        for m in order[:depth]:
            size //= 2
            at = at + bit[m] * size
        return pl.multiple_of(at, size), pl.multiple_of(c * R + core * H + at, size), size

    def scatter(q, p, stage):
        dst = (r1, r2, r3)[stage - 1]
        at = pl.ds(*COLS[q][p])
        return remote(
            out.at[pl.ds(0, H >> stage), at], dst.at[:, at], ss.at[stage, q, p], rs.at[stage, q, p], ORDERS[p][stage - 1]
        )

    def gather(c, q, p, stage):
        order = ORDERS[p]
        depth = 7 - stage
        _, row, size = rows_at(c, order, depth)
        at = pl.ds(*COLS[q][p])
        dst = y.at[pl.ds(row, size), at]
        src = out.at[pl.ds(0, size), at] if stage == 4 else dst
        return remote(src, dst, ss.at[stage, q, p], rs.at[stage, q, p], order[depth - 1])

    def keep(c, q, p):
        _, row, size = rows_at(c, ORDERS[p], 3)
        at = pl.ds(*COLS[q][p])
        return pltpu.make_async_copy(out.at[pl.ds(0, size), at], y.at[pl.ds(row, size), at], lsem.at[q, p])

    def last(c, q):
        row = pl.multiple_of(c * R + core * H, H)
        at = pl.ds(COLS[q][0][0], sum(w for _, w in COLS[q]))
        piece = y.at[pl.ds(row, H), at]
        return remote(piece, piece, ss.at[7, q, 0], rs.at[7, q, 0], 1)

    def act(c, q, stage):
        if stage <= 4:
            for p in range(3):
                order = ORDERS[p]
                at = pl.ds(*COLS[q][p])
                base, _, size = rows_at(c, order, stage - 1)
                if stage > 1:
                    scatter(q, p, stage - 1).wait()
                got = (None, r1, r2, r3)[stage - 1]
                if stage == 4:
                    out[pl.ds(0, size), at] = (acc[pl.ds(base, size), at] + got[:, at].astype(F32)).astype(BF16)
                    keep(c, q, p).start()
                    gather(c, q, p, 4).start()
                    continue
                half = size // 2
                b = bit[order[stage - 1]]
                give = pl.multiple_of((1 - b) * half, half)
                hold = pl.multiple_of(b * half, half)
                to = pl.ds(0, half)
                sums = acc[pl.ds(pl.multiple_of(base + give, half), half), at]
                if stage == 1:
                    out[to, at] = sums.astype(BF16)
                else:
                    out[to, at] = (sums + got[pl.ds(give, half), at].astype(F32)).astype(BF16)
                scatter(q, p, stage).start()
                if stage > 1:
                    mine = pl.ds(pl.multiple_of(base + hold, half), half)
                    acc[mine, at] = acc[mine, at] + got[pl.ds(hold, half), at].astype(F32)
        elif stage <= 7:
            for p in range(3):
                gather(c, q, p, stage - 1).wait()
                if stage == 5:
                    keep(c, q, p).wait()
                if stage < 7:
                    gather(c, q, p, stage).start()
            if stage == 7:
                last(c, q).start()
        else:
            last(c, q).wait()

    def round_(c, n):
        for q in range(PIECES):
            stage = 4 - q + n
            if 1 <= stage <= 8:
                act(c, q, stage)

    barrier = pltpu.get_barrier_semaphore()
    for m in (1, 2, 4, 8):
        pl.semaphore_signal(barrier, inc=1, device_id={"tp": peer[m]}, device_id_type=MESH)
    start(load_x(0))
    start(load_gu(0, 0))
    pl.semaphore_wait(barrier, 4)

    ROUNDS = {1: 1, 3: 2, 5: 3, 7: 4, 9: 5, 10: 6}

    def chunk(c, _):
        wait(load_x(c))

        def gate_up(j, _):
            slot = lax.rem(j, 2)

            @pl.when(j < ng - 1)
            def _():
                start(load_gu(j + 1, 1 - slot))

            @pl.when(j == 0)
            def _():
                start(load_d(0, 0))

            wait(load_gu(j, slot))
            gate = jnp.dot(xb[...], gb[slot], preferred_element_type=F32)
            up = jnp.dot(xb[...], ub[slot], preferred_element_type=F32)
            h[:, pl.ds(pl.multiple_of(j * TN, TN), TN)] = (jax.nn.silu(gate) * up).astype(BF16)

            for step, n in ROUNDS.items():
                @pl.when((c > 0) & (j == step))
                def _():
                    round_(c - 1, n)
            return 0

        lax.fori_loop(0, ng, gate_up, 0)

        def down(k, _):
            slot = lax.rem(k, 2)

            @pl.when(k < nd - 1)
            def _():
                start(load_d(k + 1, 1 - slot))

            @pl.when((k == 0) & (c < nc - 1))
            def _():
                start(load_gu(0, 0))
                start(load_x(c + 1))

            wait(load_d(k, slot))
            term = jnp.dot(h[...], db[slot], preferred_element_type=F32)

            @pl.when(k > 0)
            def _():
                finish0(k - 1)

            acc[:, pl.ds(pl.multiple_of(k * TD, TD), TD)] = term[:H]
            oth[...] = term[H:].astype(BF16)
            stage0(k).start()

            @pl.when((k == 1) & (c > 0))
            def _():
                round_(c - 1, 7)

            for step, n in ((2, -3), (4, -2), (6, -1)):
                @pl.when(k == step)
                def _():
                    round_(c, n)
            return 0

        lax.fori_loop(0, nd, down, 0)
        finish0(nd - 1)
        round_(c, 0)
        return 0

    lax.fori_loop(0, nc, chunk, 0)
    for n in range(1, 8):
        round_(nc - 1, n)


def solution(mesh):
    def step(x, w_gate, w_up, w_down):
        rows, d = x.shape
        ff = w_gate.shape[1]
        hbm = pl.BlockSpec(memory_space=pl.ANY)
        dma = pltpu.SemaphoreType.DMA
        return pl.pallas_call(
            kernel,
            out_shape=jax.ShapeDtypeStruct((rows, d), BF16),
            in_specs=[hbm] * 4,
            out_specs=hbm,
            scratch_shapes=[
                pltpu.VMEM((R, d), BF16),
                pltpu.VMEM((2, d, TN), BF16),
                pltpu.VMEM((2, d, TN), BF16),
                pltpu.VMEM((2, ff, TD), BF16),
                pltpu.VMEM((R, ff), BF16),
                pltpu.VMEM((H, d), F32),
                pltpu.VMEM((H, TD), BF16),
                pltpu.VMEM((2, H, TD), BF16),
                pltpu.VMEM((H // 2, d), BF16),
                pltpu.VMEM((H // 2, d), BF16),
                pltpu.VMEM((H // 4, d), BF16),
                pltpu.VMEM((H // 8, d), BF16),
                dma((2,)),
                dma((2,)),
                dma((2,)),
                dma((2,)),
                dma((2,)),
                dma((2,)),
                dma((8, PIECES, 3)),
                dma((8, PIECES, 3)),
                dma((PIECES, 3)),
            ],
            compiler_params=pltpu.CompilerParams(
                collective_id=0, has_side_effects=True, vmem_limit_bytes=67_000_000
            ),
        )(x, w_gate, w_up, w_down)

    return jax.shard_map(
        step,
        mesh=mesh,
        in_specs=(P("dp", None), P(None, "tp"), P(None, "tp"), P("tp", None)),
        out_specs=P("dp", None),
        check_vma=False,
    )
```

```python
import jax
import jax.numpy as jnp
from jax import lax
from jax.experimental import pallas as pl
from jax.experimental.pallas import tpu as pltpu
from jax.sharding import PartitionSpec as P

MESH = pl.DeviceIdType.MESH
BF16, F32 = jnp.bfloat16, jnp.float32

R = 512
H = R // 2
TN = 256
TD = 1024
PIECES = 8
ORDERS = ((8, 4, 2), (4, 2, 8), (2, 8, 4))
TILES = ((3, 3, 2), (3, 2, 3), (2, 3, 3))

AFTER_DOWN = tuple(
    tuple((q, s) for s in (4, 3, 2, 1) for q in [k + 1 - 2 * s] if q >= 0) for k in range(PIECES)
)
ROUNDS = (
    ((7, 1), (5, 2), (6, 2), (3, 3), (4, 3), (1, 4), (2, 4), (0, 5)),
    ((7, 2), (5, 3), (6, 3), (3, 4), (4, 4), (1, 5), (2, 5), (0, 6)),
    ((7, 3), (5, 4), (6, 4), (3, 5), (4, 5), (1, 6), (2, 6), (0, 7)),
    ((7, 4), (5, 5), (6, 5), (3, 6), (1, 7), (2, 7), (0, 8)),
    ((7, 5), (4, 6), (5, 6), (3, 7), (1, 8), (2, 8)),
    ((7, 6), (6, 6), (4, 7), (5, 7), (3, 8)),
    ((7, 7), (6, 7), (4, 8), (5, 8)),
    ((6, 8), (7, 8)),
)
AFTER_GATE_UP = (0, 2, 4, 6, 8, 10, 11)


def part_columns():
    out, at = [], 0
    for q in range(PIECES):
        piece = []
        for t in TILES[q % 3]:
            piece.append((at, t * 128))
            at += t * 128
        out.append(piece)
    return out


COLS = part_columns()


def kernel(
    x, wg, wu, wd, y,
    xb, gb, ub, db, h, acc, oth, r0, out, r1, r2, r3,
    xsem, gsem, usem, dsem, s0s, s0r, ss, rs, lsem,
):
    rows, d = x.shape
    nc = rows // R
    ng = wg.shape[1] // TN
    nd = d // TD
    me = lax.axis_index("tp")
    bit = {m: lax.rem(me // m, 2) for m in (1, 2, 4, 8)}
    peer = {m: me + m - 2 * m * bit[m] for m in (1, 2, 4, 8)}
    core = bit[1]

    def remote(src, dst, ssem, rsem, mask):
        return pltpu.make_async_remote_copy(
            src_ref=src, dst_ref=dst, send_sem=ssem, recv_sem=rsem,
            device_id={"tp": peer[mask]}, device_id_type=MESH,
        )

    def load_x(c):
        own = pl.multiple_of(c * R + core * H, H)
        other = pl.multiple_of(c * R + (1 - core) * H, H)
        return (
            pltpu.make_async_copy(x.at[pl.ds(own, H)], xb.at[pl.ds(0, H)], xsem.at[0]),
            pltpu.make_async_copy(x.at[pl.ds(other, H)], xb.at[pl.ds(H, H)], xsem.at[1]),
        )

    def load_gu(j, slot):
        at = pl.ds(pl.multiple_of(j * TN, TN), TN)
        return (
            pltpu.make_async_copy(wg.at[:, at], gb.at[slot], gsem.at[slot]),
            pltpu.make_async_copy(wu.at[:, at], ub.at[slot], usem.at[slot]),
        )

    def load_d(k, slot):
        at = pl.ds(pl.multiple_of(k * TD, TD), TD)
        return (pltpu.make_async_copy(wd.at[:, at], db.at[slot], dsem.at[slot]),)

    def start(copies):
        for c in copies:
            c.start()

    def wait(copies):
        for c in copies:
            c.wait()

    def stage0(k):
        slot = lax.rem(k, 2)
        return remote(oth.at[slot], r0.at[slot], s0s.at[slot], s0r.at[slot], 1)

    def finish0(k):
        stage0(k).wait()
        at = pl.ds(pl.multiple_of(k * TD, TD), TD)
        acc[:, at] = acc[:, at] + r0[lax.rem(k, 2)].astype(F32)

    def rows_at(c, order, depth):
        at, size = 0, H
        for m in order[:depth]:
            size //= 2
            at = at + bit[m] * size
        return pl.multiple_of(at, size), pl.multiple_of(c * R + core * H + at, size), size

    def scatter(q, p, stage):
        dst = (r1, r2, r3)[stage - 1]
        at = pl.ds(*COLS[q][p])
        return remote(
            out.at[pl.ds(0, H >> stage), at], dst.at[:, at], ss.at[stage, q, p], rs.at[stage, q, p], ORDERS[p][stage - 1]
        )

    def gather(c, q, p, stage):
        order = ORDERS[p]
        depth = 7 - stage
        _, row, size = rows_at(c, order, depth)
        at = pl.ds(*COLS[q][p])
        dst = y.at[pl.ds(row, size), at]
        src = out.at[pl.ds(0, size), at] if stage == 4 else dst
        return remote(src, dst, ss.at[stage, q, p], rs.at[stage, q, p], order[depth - 1])

    def keep(c, q, p):
        _, row, size = rows_at(c, ORDERS[p], 3)
        at = pl.ds(*COLS[q][p])
        return pltpu.make_async_copy(out.at[pl.ds(0, size), at], y.at[pl.ds(row, size), at], lsem.at[q, p])

    def last(c, q):
        row = pl.multiple_of(c * R + core * H, H)
        at = pl.ds(COLS[q][0][0], sum(w for _, w in COLS[q]))
        piece = y.at[pl.ds(row, H), at]
        return remote(piece, piece, ss.at[7, q, 0], rs.at[7, q, 0], 1)

    def act(c, q, stage):
        if stage <= 4:
            for p in range(3):
                order = ORDERS[p]
                at = pl.ds(*COLS[q][p])
                base, _, size = rows_at(c, order, stage - 1)
                if stage > 1:
                    scatter(q, p, stage - 1).wait()
                got = (None, r1, r2, r3)[stage - 1]
                if stage == 4:
                    out[pl.ds(0, size), at] = (acc[pl.ds(base, size), at] + got[:, at].astype(F32)).astype(BF16)
                    keep(c, q, p).start()
                    gather(c, q, p, 4).start()
                    continue
                half = size // 2
                b = bit[order[stage - 1]]
                give = pl.multiple_of((1 - b) * half, half)
                hold = pl.multiple_of(b * half, half)
                to = pl.ds(0, half)
                sums = acc[pl.ds(pl.multiple_of(base + give, half), half), at]
                if stage == 1:
                    out[to, at] = sums.astype(BF16)
                else:
                    out[to, at] = (sums + got[pl.ds(give, half), at].astype(F32)).astype(BF16)
                scatter(q, p, stage).start()
                if stage > 1:
                    mine = pl.ds(pl.multiple_of(base + hold, half), half)
                    acc[mine, at] = acc[mine, at] + got[pl.ds(hold, half), at].astype(F32)
        elif stage <= 7:
            for p in range(3):
                gather(c, q, p, stage - 1).wait()
                if stage == 5:
                    keep(c, q, p).wait()
                if stage < 7:
                    gather(c, q, p, stage).start()
            if stage == 7:
                last(c, q).start()
        else:
            last(c, q).wait()

    def acts(c, pairs):
        for q, stage in pairs:
            act(c, q, stage)

    barrier = pltpu.get_barrier_semaphore()
    for m in (1, 2, 4, 8):
        pl.semaphore_signal(barrier, inc=1, device_id={"tp": peer[m]}, device_id_type=MESH)
    start(load_x(0))
    start(load_gu(0, 0))
    pl.semaphore_wait(barrier, 4)

    def chunk(c, _):
        wait(load_x(c))

        def gate_up(j, _):
            slot = lax.rem(j, 2)

            @pl.when(j < ng - 1)
            def _():
                start(load_gu(j + 1, 1 - slot))

            @pl.when(j == 0)
            def _():
                start(load_d(0, 0))

            wait(load_gu(j, slot))
            gate = jnp.dot(xb[...], gb[slot], preferred_element_type=F32)
            up = jnp.dot(xb[...], ub[slot], preferred_element_type=F32)
            h[:, pl.ds(pl.multiple_of(j * TN, TN), TN)] = (jax.nn.silu(gate) * up).astype(BF16)

            for step, pairs in zip(AFTER_GATE_UP, ROUNDS):
                @pl.when((c > 0) & (j == step))
                def _():
                    if step == AFTER_GATE_UP[0]:
                        finish0(nd - 1)
                    acts(c - 1, pairs)
            return 0

        lax.fori_loop(0, ng, gate_up, 0)

        def down(k, _):
            slot = lax.rem(k, 2)

            @pl.when(k < nd - 1)
            def _():
                start(load_d(k + 1, 1 - slot))

            @pl.when((k == 0) & (c < nc - 1))
            def _():
                start(load_gu(0, 0))
                start(load_x(c + 1))

            wait(load_d(k, slot))
            term = jnp.dot(h[...], db[slot], preferred_element_type=F32)

            acc[:, pl.ds(pl.multiple_of(k * TD, TD), TD)] = term[:H]
            oth[slot] = term[H:].astype(BF16)

            @pl.when(k > 0)
            def _():
                finish0(k - 1)

            stage0(k).start()

            @pl.when((k == 0) & (c > 0))
            def _():
                acts(c - 1, ROUNDS[-1])

            for step, pairs in enumerate(AFTER_DOWN):
                if pairs:
                    @pl.when(k == step)
                    def _():
                        acts(c, pairs)
            return 0

        lax.fori_loop(0, nd, down, 0)
        return 0

    lax.fori_loop(0, nc, chunk, 0)
    finish0(nd - 1)
    for pairs in ROUNDS:
        acts(nc - 1, pairs)


def solution(mesh):
    def step(x, w_gate, w_up, w_down):
        rows, d = x.shape
        ff = w_gate.shape[1]
        hbm = pl.BlockSpec(memory_space=pl.ANY)
        dma = pltpu.SemaphoreType.DMA
        return pl.pallas_call(
            kernel,
            out_shape=jax.ShapeDtypeStruct((rows, d), BF16),
            in_specs=[hbm] * 4,
            out_specs=hbm,
            scratch_shapes=[
                pltpu.VMEM((R, d), BF16),
                pltpu.VMEM((2, d, TN), BF16),
                pltpu.VMEM((2, d, TN), BF16),
                pltpu.VMEM((2, ff, TD), BF16),
                pltpu.VMEM((R, ff), BF16),
                pltpu.VMEM((H, d), F32),
                pltpu.VMEM((2, H, TD), BF16),
                pltpu.VMEM((2, H, TD), BF16),
                pltpu.VMEM((H // 2, d), BF16),
                pltpu.VMEM((H // 2, d), BF16),
                pltpu.VMEM((H // 4, d), BF16),
                pltpu.VMEM((H // 8, d), BF16),
                dma((2,)),
                dma((2,)),
                dma((2,)),
                dma((2,)),
                dma((2,)),
                dma((2,)),
                dma((8, PIECES, 3)),
                dma((8, PIECES, 3)),
                dma((PIECES, 3)),
            ],
            compiler_params=pltpu.CompilerParams(
                collective_id=0, has_side_effects=True, vmem_limit_bytes=67_000_000
            ),
        )(x, w_gate, w_up, w_down)

    return jax.shard_map(
        step,
        mesh=mesh,
        in_specs=(P("dp", None), P(None, "tp"), P(None, "tp"), P("tp", None)),
        out_specs=P("dp", None),
        check_vma=False,
    )
```
